256 devices in a mesh: dp: 64 (over z, x, core), tensor: 4 (over y).
Axes of the slice: x: 4, y: 4, z: 8, core: 2. Of those that a mesh axis runs over, the one named last changes fastest.
Arguments:
- prefix: bfloat16 [64, 128, 8192], P('dp'), may hold values from -6 to 6
- kv_weight: bfloat16 [8192, 2, 512], P(None, None, 'tensor'), may hold values from -0.044194174 to 0.044194174
- ans_query: bfloat16 [65536, 4096], P('dp', 'tensor'), may hold values from -60 to 60
- ans_kv: bfloat16 [65536, 2, 512], P('dp', None, 'tensor'), may hold values from -8 to 8
- d_out: bfloat16 [65536, 4096], P('dp', 'tensor'), may hold values from -192 to 192
- branch_prompt: int32 [128], P('dp'), may hold values from 0 to 63, as said below
Outputs:
- attn_out: bfloat16 [65536, 4096], P('dp', 'tensor')
- prefix_grad: bfloat16 [64, 128, 8192], P('dp', 'tensor')
The draws below stay inside these ranges and needn't reach their ends.
Inputs may be any that keep to these rules, and one draw needn't show every extreme that they name: `branch_prompt`: prompt p is owned by dp index p. The dp index that holds a branch and the owner of its prompt are at most 3 steps apart, counting around the axis. Every dp index holds at least one answer to its own prompt.
All inputs are finite; a program needn't handle non-finite values.
Results may differ from the reference program's by a relative error of at most 0.014.
The reference program's roundings to bfloat16 on the way count: a program that leaves them out, or rounds other values in their place, can miss the bound.
Values may be sent and summed in bfloat16 or wider, within the bound.
A program may use at most 128 MiB of HBM per device.

```python
import math
import jax
import jax.numpy as jnp
from jax import lax

D = 8192
QH = 32
KVH = 4
HD = 128
PFX = 128
ANS = 512
BR_DEV = 2
REACH = 3
PROMPTS = 64
BRANCHES = 128
TOKENS = 65536


def weight_draw(key):
    normal_part = jax.random.truncated_normal(jax.random.fold_in(key, 31), -4.0, 4.0, (D, 2, KVH * HD), jnp.float32)
    return normal_part * (1.0 / math.sqrt(D))


def draw_kv_weight(key, part):
    return weight_draw(key).astype(jnp.bfloat16)


def draw_prefix(key, part):
    values = jax.random.truncated_normal(jax.random.fold_in(key, 43), -6.0, 6.0, (PROMPTS, PFX, D), jnp.float32)
    return values.astype(jnp.bfloat16)


def answer_pair(key):
    groups = QH // KVH
    queries = jax.random.truncated_normal(jax.random.fold_in(key, 21), -6.0, 6.0, (BRANCHES, ANS, KVH, groups, HD), jnp.float32)
    key_rows = jax.random.truncated_normal(jax.random.fold_in(key, 22), -6.0, 6.0, (BRANCHES, ANS, KVH, HD), jnp.float32)
    value_rows = jax.random.truncated_normal(jax.random.fold_in(key, 23), -6.0, 6.0, (BRANCHES, ANS, KVH, HD), jnp.float32)
    return (queries, key_rows, value_rows)


def draw_ans_query(key, part):
    queries, key_rows, value_rows = answer_pair(key)
    return queries.reshape(TOKENS, QH * HD).astype(jnp.bfloat16)


def draw_ans_kv(key, part):
    queries, key_rows, value_rows = answer_pair(key)
    return jnp.stack([key_rows, value_rows], axis=2).reshape(TOKENS, 2, KVH * HD).astype(jnp.bfloat16)


def draw_branch_prompt(key, part):
    devices = jnp.arange(PROMPTS)
    offsets = jax.random.randint(jax.random.fold_in(key, 11), (PROMPTS, BR_DEV), -REACH, REACH + 1)
    own_slot = jax.random.randint(jax.random.fold_in(key, 12), (PROMPTS,), 0, BR_DEV)
    shuffled = jax.random.permutation(jax.random.fold_in(key, 13), PROMPTS)
    listed = jnp.arange(2 * REACH)
    listed = jnp.where(listed < REACH, listed - REACH, listed - REACH + 1)
    forced = jnp.zeros((PROMPTS,), jnp.int32).at[shuffled[:2 * REACH]].set(listed.astype(jnp.int32))
    has_forced = jnp.zeros((PROMPTS,), jnp.int32).at[shuffled[:2 * REACH]].set(1)
    slot_ids = jnp.arange(BR_DEV)
    second_slot = (own_slot + 1) % BR_DEV
    forced_here = (slot_ids[None, :] == second_slot[:, None]) & (has_forced[:, None] == 1)
    offsets = jnp.where(forced_here, forced[:, None], offsets)
    offsets = jnp.where(slot_ids[None, :] == own_slot[:, None], 0, offsets)
    return ((devices[:, None] + offsets) % PROMPTS).reshape(BRANCHES).astype(jnp.int32)


def steps_of(key, shape, shards, low, high):
    loudness, own = 1.0, jax.random.fold_in(key, 6)
    for axis_at, shards_of in shards:
        heights = jnp.exp(jax.random.uniform(jax.random.fold_in(own, axis_at), (shards_of,), jnp.float32, low / len(shards), high / len(shards)))
        loudness = loudness * jnp.repeat(heights, shape[axis_at] // shards_of).reshape([-1 if axis == axis_at else 1 for axis in range(len(shape))])
    return loudness


def gaussian(own_key, extent, scale, bound, split=(), dtype=jnp.bfloat16):
    loudness = steps_of(own_key, extent, split, -0.22, 0.18) if split else 1.0
    entries = jax.random.normal(own_key, extent, jnp.float32) * scale * loudness
    return jnp.minimum(jnp.maximum(entries, -bound), bound).astype(dtype)


def setup_inputs(seed: int = 0) -> dict:
    key_list = jax.random.split(jax.random.key(seed), 7)
    prefix = draw_prefix(jax.random.fold_in(key_list[6], 71), 0)
    kv_weight = draw_kv_weight(jax.random.fold_in(key_list[6], 71), 0)
    ans_query = draw_ans_query(jax.random.fold_in(key_list[6], 71), 0)
    ans_kv = draw_ans_kv(jax.random.fold_in(key_list[6], 71), 0)
    d_out = gaussian(key_list[4], (TOKENS, QH * HD), 32.0, 192.0, ((0, 64), (1, 4)))
    branch_prompt = draw_branch_prompt(jax.random.fold_in(key_list[6], 71), 0)
    return dict(prefix=prefix, kv_weight=kv_weight, ans_query=ans_query, ans_kv=ans_kv, d_out=d_out, branch_prompt=branch_prompt)


def branch_pass(queries, key_rows, value_rows, upstream):
    answers = queries.shape[0]
    prefix_len = key_rows.shape[0] - answers
    scaling = queries.shape[-1] ** -0.5
    query_f = queries.astype(jnp.float32)
    key_f = key_rows.astype(jnp.float32)
    value_f = value_rows.astype(jnp.float32)
    upstream_f = upstream.astype(jnp.float32)
    scores = jnp.einsum("ahgd,khd->hgak", query_f, key_f) * scaling
    key_pos = jnp.arange(key_rows.shape[0])
    row_pos = jnp.arange(answers)
    allowed = (key_pos[None, :] < prefix_len) | (key_pos[None, :] - prefix_len <= row_pos[:, None])
    scores = jnp.where(allowed, scores, -jnp.inf)
    row_max = jnp.max(scores, axis=-1, keepdims=True)
    exps = jnp.exp(scores - row_max)
    prob_full = exps / jnp.sum(exps, axis=-1, keepdims=True)
    prob_half = lax.optimization_barrier(prob_full.astype(jnp.bfloat16)).astype(jnp.float32)
    context = jnp.einsum("hgak,khd->ahgd", prob_half, value_f)
    prob_grad = jnp.einsum("ahgd,khd->hgak", upstream_f, value_f)
    delta_row = jnp.einsum("ahgd,ahgd->hga", upstream_f, context)
    score_grad = prob_full * (prob_grad - delta_row[..., None])
    score_half = lax.optimization_barrier(score_grad.astype(jnp.bfloat16)).astype(jnp.float32)
    key_grad = jnp.einsum("hgak,ahgd->khd", score_half[..., :prefix_len], query_f) * scaling
    value_grad = jnp.einsum("hgak,ahgd->khd", prob_half[..., :prefix_len], upstream_f)
    return context.astype(jnp.bfloat16), key_grad, value_grad


def reference(prefix, kv_weight, ans_query, ans_kv, d_out, branch_prompt):
    groups = QH // KVH
    flat_weight = kv_weight.reshape(D, 2 * KVH * HD)

    def project(prompt_rows):
        return jnp.dot(prompt_rows, flat_weight, preferred_element_type=jnp.float32).astype(jnp.bfloat16)

    prompt_kv = lax.map(project, prefix).reshape(PROMPTS, PFX, 2, KVH, HD)
    queries = ans_query.reshape(BRANCHES, ANS, KVH, groups, HD)
    answer_kv = ans_kv.reshape(BRANCHES, ANS, 2, KVH, HD)
    upstream = d_out.reshape(BRANCHES, ANS, KVH, groups, HD)

    def one_branch(packed):
        branch_q, branch_kv, branch_up, prompt_id = packed
        own_kv = lax.dynamic_index_in_dim(prompt_kv, prompt_id.astype(jnp.int32), 0, keepdims=False)
        key_rows = jnp.concatenate([own_kv[:, 0], branch_kv[:, 0]], axis=0)
        value_rows = jnp.concatenate([own_kv[:, 1], branch_kv[:, 1]], axis=0)
        return branch_pass(branch_q, key_rows, value_rows, branch_up)

    context, key_grad, value_grad = lax.map(one_branch, (queries, answer_kv, upstream, branch_prompt))
    attn_out = context.reshape(TOKENS, QH * HD)
    both_grads = jnp.stack([key_grad, value_grad], axis=2).reshape(BRANCHES, PFX * 2 * KVH * HD)
    kv_sum = jax.ops.segment_sum(both_grads, branch_prompt, num_segments=PROMPTS)
    kv_grad = kv_sum.astype(jnp.bfloat16).reshape(PROMPTS, PFX, 2 * KVH * HD)

    def project_back(grad_rows):
        return lax.dot_general(grad_rows, flat_weight, (((1,), (1,)), ((), ())), preferred_element_type=jnp.float32).astype(jnp.bfloat16)

    prefix_grad = lax.map(project_back, kv_grad)
    return attn_out, prefix_grad
```

```python
import functools
import math

import jax
import jax.numpy as jnp
from jax import lax
from jax.experimental import pallas as pl
from jax.experimental.pallas import tpu as pltpu
from jax.sharding import PartitionSpec as P

MESH = pl.DeviceIdType.MESH
HD = 128
PFX = 128
ANS = 512
HEADS = 8
D = 8192
REACH = 3
WINDOW = 2 * REACH + 1
CHUNK = 512
CHUNKS = D // CHUNK
COLS = 1024
ROWS = 256
FIRST = 4
SCALING = HD ** (-0.5)
LOG2E = math.log2(math.e)
OFFSETS = [o for o in (3, -3, 2, -2, 1, -1)]
f32, bf16 = jnp.float32, jnp.bfloat16


def dot(a, b, dims):
    return lax.dot_general(a, b, (dims, ((), ())), preferred_element_type=f32)


def kernel(
    dp_count,
    t_count,
    bp_ref,
    prefix_hbm,
    w_hbm,
    q_hbm,
    kv_hbm,
    do_hbm,
    attn_hbm,
    pg_hbm,
    prefix_v,
    w_v,
    q_v,
    do_v,
    kv_v,
    wide,
    acc,
    near,
    kfull,
    vfull,
    res,
    kg,
    gsend,
    grecv,
    gbuf,
    wbuf,
    wfull,
    otile,
    load_sem,
    in_sem,
    out_sem,
    kv_send,
    kv_recv,
    w_send,
    w_recv,
    gr_send,
    gr_recv,
    gt_send,
    gt_recv,
    pg_send,
    pg_recv,
):
    d = lax.axis_index("dp")
    t = lax.axis_index("tensor")
    core = lax.rem(d, 2)
    sib = d + 1 - 2 * core
    unit = t * 2 + core

    def dp_at(by):
        return lax.rem(d + by + dp_count, dp_count)

    def t_at(by):
        return lax.rem(t + by, t_count)

    loads = []
    for c in range(CHUNKS):
        cols = pl.ds(c * CHUNK, CHUNK)
        rows = pl.ds(c * 2 * CHUNK, 2 * CHUNK)
        pltpu.make_async_copy(prefix_hbm.at[:, cols], prefix_v.at[:, cols], load_sem.at[0, c]).start()
        pltpu.make_async_copy(w_hbm.at[rows], w_v.at[rows], load_sem.at[1, c]).start()
    for n, (src, dst) in enumerate(((kv_hbm, kv_v), (q_hbm, q_v), (do_hbm, do_v))):
        cp = pltpu.make_async_copy(src, dst, in_sem.at[n])
        cp.start()
        loads.append(cp)

    barrier = pltpu.get_barrier_semaphore()
    for o in OFFSETS:
        pl.semaphore_signal(barrier, inc=1, device_id={"dp": dp_at(o), "tensor": t}, device_id_type=MESH)
    for by in range(1, 4):
        pl.semaphore_signal(barrier, inc=1, device_id={"dp": d, "tensor": t_at(by)}, device_id_type=MESH)
        pl.semaphore_signal(barrier, inc=1, device_id={"dp": sib, "tensor": t_at(by)}, device_id_type=MESH)
    pl.semaphore_wait(barrier, 12)

    w_copies = []
    for by in (2, 1, 3):
        to = t_at(by)
        rows = pl.ds(pl.multiple_of((to * 2 + core) * 2 * COLS, 2 * COLS), 2 * COLS)
        cp = pltpu.make_async_remote_copy(
            src_ref=w_hbm.at[rows],
            dst_ref=wbuf.at[by - 1],
            send_sem=w_send.at[by - 1],
            recv_sem=w_recv.at[by - 1],
            device_id={"dp": d, "tensor": to},
            device_id_type=MESH,
        )
        cp.start()
        w_copies.append(cp)

    def halves(block, n):
        wide[pl.ds(0, 2 * n), :] = block.astype(f32)
        even = wide[pl.ds(0, n, stride=2), :].astype(bf16)
        odd = wide[pl.ds(1, n, stride=2), :].astype(bf16)
        return even, odd

    acc[...] = jnp.zeros_like(acc)

    def project(c, carry):
        cols = pl.ds(pl.multiple_of(c * CHUNK, CHUNK), CHUNK)
        rows = pl.ds(pl.multiple_of(c * 2 * CHUNK, 2 * CHUNK), 2 * CHUNK)
        pltpu.make_async_copy(prefix_hbm.at[:, cols], prefix_v.at[:, cols], load_sem.at[0, c]).wait()
        pltpu.make_async_copy(w_hbm.at[rows], w_v.at[rows], load_sem.at[1, c]).wait()
        wk, wv = halves(w_v[rows, :], CHUNK)
        acc[...] += dot(prefix_v[:, cols], jnp.concatenate([wk, wv], axis=1), ((1,), (0,)))
        return carry

    lax.fori_loop(0, CHUNKS, project, 0)
    near[REACH] = acc[...].astype(bf16)

    kv_copies = []
    for n, o in enumerate(OFFSETS):
        cp = pltpu.make_async_remote_copy(
            src_ref=near.at[REACH],
            dst_ref=near.at[REACH - o],
            send_sem=kv_send.at[n],
            recv_sem=kv_recv.at[n],
            device_id={"dp": dp_at(o), "tensor": t},
            device_id_type=MESH,
        )
        cp.start()
        kv_copies.append(cp)

    first_own = bp_ref[0] == d
    own_slot = jnp.where(first_own, 0, 1)
    other_slot = 1 - own_slot
    other_index = lax.rem(jnp.where(first_own, bp_ref[1], bp_ref[0]) - d + REACH + dp_count, dp_count)

    for cp in loads:
        cp.wait()

    def take_answers(role, slot):
        keys, values = halves(kv_v[slot], ANS)
        kfull[role, pl.ds(PFX, ANS), :] = keys
        vfull[role, pl.ds(PFX, ANS), :] = values

    def take_prefix(role, block):
        kfull[role, pl.ds(0, PFX), :] = block[:, :HD]
        vfull[role, pl.ds(0, PFX), :] = block[:, HD:]

    take_answers(0, own_slot)
    take_answers(1, other_slot)
    take_prefix(0, near[REACH])
    kg[...] = jnp.zeros_like(kg)

    def attend(n, carry):
        @pl.when(n == FIRST)
        def _():
            for cp in kv_copies:
                cp.wait()
            take_prefix(1, near[jnp.minimum(other_index, WINDOW - 1)])

        is_other = (n >= FIRST) & (n < FIRST + HEADS)
        role = jnp.where(is_other, 1, 0)
        head = jnp.where(n < FIRST, n, jnp.where(is_other, n - FIRST, n - HEADS))
        slot = jnp.where(is_other, other_slot, own_slot)
        lanes = pl.ds(pl.multiple_of(head * HD, HD), HD)
        for i in range(ANS // ROWS):
            rows = pl.ds(i * ROWS, ROWS)
            keys = PFX + (i + 1) * ROWS
            q = q_v[slot, rows, lanes]
            do = do_v[slot, rows, lanes]
            s = dot(q, kfull[role, pl.ds(0, keys), :], ((1,), (1,)))
            row_at = lax.broadcasted_iota(jnp.int32, (ROWS, ROWS), 0)
            key_at = lax.broadcasted_iota(jnp.int32, (ROWS, ROWS), 1)
            tail = jnp.where(key_at <= row_at, s[:, keys - ROWS :], -jnp.inf)
            s = jnp.concatenate([s[:, : keys - ROWS], tail], axis=1)
            top = jnp.max(s, axis=1, keepdims=True)
            e = jnp.exp2((s - top) * (SCALING * LOG2E))
            full = e * (1.0 / jnp.sum(e, axis=1, keepdims=True))
            half = full.astype(bf16)
            ctx = dot(half, vfull[role, pl.ds(0, keys), :], ((1,), (0,)))
            res[role, rows, lanes] = ctx.astype(bf16)
            grad = dot(do, vfull[role, pl.ds(0, PFX), :], ((1,), (1,)))
            delta = jnp.sum(do.astype(f32) * ctx, axis=1, keepdims=True)
            sg = (full[:, :PFX] * (grad - delta)).astype(bf16)
            kg[role, 0] += dot(sg, q, ((0,), (0,)))
            kg[role, 1] += dot(half[:, :PFX], do, ((0,), (0,)))

        @pl.when(n == FIRST + HEADS - 1)
        def _():
            key_grad = (kg[1, 0] * SCALING).astype(bf16)
            value_grad = kg[1, 1].astype(bf16)
            zero = jnp.zeros((PFX, HD), bf16)
            for m, o in enumerate(OFFSETS):
                keep = other_index == o + REACH
                gsend[m, :, pl.ds(0, HD)] = lax.select(keep, key_grad, zero)
                gsend[m, :, pl.ds(HD, HD)] = lax.select(keep, value_grad, zero)
                grad_copy(m, o).start()

        return carry

    def grad_copy(m, o):
        return pltpu.make_async_remote_copy(
            src_ref=gsend.at[m],
            dst_ref=grecv.at[m],
            send_sem=gr_send.at[m],
            recv_sem=gr_recv.at[m],
            device_id={"dp": dp_at(o), "tensor": t},
            device_id_type=MESH,
        )

    lax.fori_loop(0, 2 * HEADS, attend, 0)

    def place(b, carry):
        rows = pl.ds(pl.multiple_of(b * 64, 64), 64)
        own, other = res[0, rows, :], res[1, rows, :]
        q_v[0, rows, :] = lax.select(first_own, own, other)
        q_v[1, rows, :] = lax.select(first_own, other, own)
        return carry

    lax.fori_loop(0, ANS // 64, place, 0)
    attn_copy = pltpu.make_async_copy(q_v, attn_hbm, out_sem.at[0])
    attn_copy.start()

    local = (other_index == REACH).astype(f32)
    key_sum = (kg[0, 0] + kg[1, 0] * local) * SCALING
    value_sum = kg[0, 1] + kg[1, 1] * local
    for m, o in enumerate(OFFSETS):
        grad_copy(m, o).wait()
        key_sum = key_sum + grecv[m, :, pl.ds(0, HD)].astype(f32)
        value_sum = value_sum + grecv[m, :, pl.ds(HD, HD)].astype(f32)
    gbuf[0, 0, :, pl.ds(0, HD)] = key_sum.astype(bf16)
    gbuf[0, 0, :, pl.ds(HD, HD)] = value_sum.astype(bf16)

    gather = []
    for n, (cross, by) in enumerate(((1, 2), (0, 2), (1, 1), (0, 1), (1, 3), (0, 3), (1, 0))):
        cp = pltpu.make_async_remote_copy(
            src_ref=gbuf.at[0, 0],
            dst_ref=gbuf.at[cross, (t_count - by) % t_count],
            send_sem=gt_send.at[n],
            recv_sem=gt_recv.at[n],
            device_id={"dp": sib if cross else d, "tensor": t_at(by)},
            device_id_type=MESH,
        )
        cp.start()
        gather.append(cp)

    def widen(by, b, block):
        n = CHUNK
        wk, wv = halves(block, n)
        rows = pl.ds(b * n, n)
        wfull[rows, pl.ds(by * 2 * HD, HD)] = wk
        wfull[rows, pl.ds(by * 2 * HD + HD, HD)] = wv

    for b in range(COLS // CHUNK):
        start = pl.multiple_of(unit * 2 * COLS + b * 2 * CHUNK, 2 * CHUNK)
        widen(0, b, w_v[pl.ds(start, 2 * CHUNK), :])
    for cp in w_copies:
        cp.wait()
    for by in (1, 2, 3):
        for b in range(COLS // CHUNK):
            widen(by, b, wbuf[3 - by, pl.ds(b * 2 * CHUNK, 2 * CHUNK), :])
    for cp in gather:
        cp.wait()

    lhs = jnp.concatenate(
        [jnp.concatenate([gbuf[c, by] for by in range(4)], axis=1) for c in range(2)], axis=0
    )
    otile[...] = dot(lhs, wfull[...], ((1,), (1,))).astype(bf16).reshape(2, PFX, COLS)

    here = pl.ds(pl.multiple_of(unit * COLS, COLS), COLS)
    share = PFX // 4
    outs = []
    for n, (cross, by) in enumerate(((1, 2), (0, 2), (1, 1), (0, 1), (1, 3), (0, 3), (1, 0))):
        to = t_at(by)
        cp = pltpu.make_async_remote_copy(
            src_ref=otile.at[cross, pl.ds(pl.multiple_of(to * share, share), share)],
            dst_ref=pg_hbm.at[:, here],
            send_sem=pg_send.at[n],
            recv_sem=pg_recv.at[n],
            device_id={"dp": sib if cross else d, "tensor": to},
            device_id_type=MESH,
        )
        cp.start()
        outs.append(cp)
    mine = pltpu.make_async_copy(
        otile.at[0, pl.ds(pl.multiple_of(t * share, share), share)], pg_hbm.at[:, here], out_sem.at[1]
    )
    mine.start()
    mine.wait()
    attn_copy.wait()
    for cp in outs:
        cp.wait()


def shards(prefix, kv_weight, ans_query, ans_kv, d_out, branch_prompt):
    t_count, dp_count = lax.axis_size("tensor"), lax.axis_size("dp")
    anyspec = pl.BlockSpec(memory_space=pl.ANY)
    dma = pltpu.SemaphoreType.DMA
    vmem = pltpu.VMEM
    attn, pg = pl.pallas_call(
        functools.partial(kernel, dp_count, t_count),
        out_shape=(
            jax.ShapeDtypeStruct((2, ANS, HEADS * HD), bf16),
            jax.ShapeDtypeStruct((PFX // 4, D), bf16),
        ),
        in_specs=[pl.BlockSpec(memory_space=pltpu.SMEM)] + [anyspec] * 5,
        out_specs=(anyspec, anyspec),
        scratch_shapes=[
            vmem((PFX, D), bf16),
            vmem((2 * D, HD), bf16),
            vmem((2, ANS, HEADS * HD), bf16),
            vmem((2, ANS, HEADS * HD), bf16),
            vmem((2, 2 * ANS, HD), bf16),
            vmem((2 * CHUNK, HD), f32),
            vmem((PFX, 2 * HD), f32),
            vmem((WINDOW, PFX, 2 * HD), bf16),
            vmem((2, PFX + ANS, HD), bf16),
            vmem((2, PFX + ANS, HD), bf16),
            vmem((2, ANS, HEADS * HD), bf16),
            vmem((2, 2, PFX, HD), f32),
            vmem((2 * REACH, PFX, 2 * HD), bf16),
            vmem((2 * REACH, PFX, 2 * HD), bf16),
            vmem((2, 4, PFX, 2 * HD), bf16),
            vmem((3, 2 * COLS, HD), bf16),
            vmem((COLS, 4 * 2 * HD), bf16),
            vmem((2, PFX, COLS), bf16),
            dma((2, CHUNKS)),
            dma((3,)),
            dma((2,)),
            dma((6,)),
            dma((6,)),
            dma((3,)),
            dma((3,)),
            dma((6,)),
            dma((6,)),
            dma((7,)),
            dma((7,)),
            dma((7,)),
            dma((7,)),
        ],
        compiler_params=pltpu.CompilerParams(
            collective_id=0, has_side_effects=True, vmem_limit_bytes=60 * 1024 * 1024
        ),
        name="prefix_step",
    )(
        branch_prompt,
        prefix.reshape(PFX, D),
        kv_weight.reshape(2 * D, HD),
        ans_query.reshape(2, ANS, HEADS * HD),
        ans_kv.reshape(2, 2 * ANS, HD),
        d_out.reshape(2, ANS, HEADS * HD),
    )
    return attn.reshape(2 * ANS, HEADS * HD), pg.reshape(1, PFX // 4, D)


def solution(mesh):
    return jax.shard_map(
        shards,
        mesh=mesh,
        in_specs=(
            P("dp", None, None),
            P(None, None, "tensor"),
            P("dp", "tensor"),
            P("dp", None, "tensor"),
            P("dp", "tensor"),
            P("dp"),
        ),
        out_specs=(P("dp", "tensor"), P("dp", "tensor", None)),
        check_vma=False,
    )
```

```python
import functools
import math

import jax
import jax.numpy as jnp
from jax import lax
from jax.experimental import pallas as pl
from jax.experimental.pallas import tpu as pltpu
from jax.sharding import PartitionSpec as P

MESH = pl.DeviceIdType.MESH
HD = 128
PFX = 128
ANS = 512
HEADS = 8
D = 8192
REACH = 3
WINDOW = 2 * REACH + 1
CHUNK = 512
CHUNKS = D // CHUNK
COLS = 1024
ROWS = 256
AT_ONCE = 4
TURNS = 2
FIRST = 2
PASS_AT = 2
AHEAD = 4
X = 4
SCALING = HD ** (-0.5)
LOG2E = math.log2(math.e)
OFFSETS = [o for o in (3, -3, 2, -2, 1, -1)]
f32, bf16 = jnp.float32, jnp.bfloat16


def dot(a, b, dims):
    return lax.dot_general(a, b, (dims, ((), ())), preferred_element_type=f32)


def kernel(
    dp_count,
    t_count,
    bp_ref,
    prefix_hbm,
    w_hbm,
    q_hbm,
    kv_hbm,
    do_hbm,
    res,
    pg,
    prefix_v,
    w_v,
    q_v,
    do_v,
    kv_v,
    wide,
    acc,
    near,
    kfull,
    vt,
    vpre,
    kg,
    gsend,
    grecv,
    gbuf,
    wbuf,
    wfull,
    otile,
    load_sem,
    in_sem,
    kv_send,
    kv_recv,
    w_send,
    w_recv,
    pass_send,
    pass_recv,
    gr_send,
    gr_recv,
    gt_send,
    gt_recv,
    pg_send,
    pg_recv,
):
    d = lax.axis_index("dp")
    t = lax.axis_index("tensor")
    core = lax.rem(d, 2)
    sib = d + 1 - 2 * core
    unit = t * 2 + core

    def dp_at(by):
        return lax.rem(d + by + dp_count, dp_count)

    def t_at(by):
        return lax.rem(t + by, t_count)

    loads = []
    for c in range(CHUNKS):
        cols = pl.ds(c * CHUNK, CHUNK)
        rows = pl.ds(c * 2 * CHUNK, 2 * CHUNK)
        pltpu.make_async_copy(prefix_hbm.at[:, cols], prefix_v.at[:, cols], load_sem.at[0, c]).start()
        pltpu.make_async_copy(w_hbm.at[rows], w_v.at[rows], load_sem.at[1, c]).start()
    for n, (src, dst) in enumerate(((kv_hbm, kv_v), (q_hbm, q_v), (do_hbm, do_v))):
        cp = pltpu.make_async_copy(src, dst, in_sem.at[n])
        cp.start()
        loads.append(cp)

    chip = d // 2
    x, z = lax.rem(chip, X), chip // X
    quarter = lax.rem(z + 2 * x, 4)
    x_next = (z * X + lax.rem(x + 1, X)) * 2 + core
    x_last = (z * X + lax.rem(x + X - 1, X)) * 2 + core
    beside = (dp_at(2 * X), dp_at(-2 * X), x_next, x_last)

    barrier = pltpu.get_barrier_semaphore()
    for o in OFFSETS:
        pl.semaphore_signal(barrier, inc=1, device_id={"dp": dp_at(o), "tensor": t}, device_id_type=MESH)
    for by in range(1, 4):
        pl.semaphore_signal(barrier, inc=1, device_id={"dp": d, "tensor": t_at(by)}, device_id_type=MESH)
        pl.semaphore_signal(barrier, inc=1, device_id={"dp": sib, "tensor": t_at(by)}, device_id_type=MESH)
    for to in beside:
        pl.semaphore_signal(barrier, inc=1, device_id={"dp": to, "tensor": t}, device_id_type=MESH)
    def halves(block, n):
        wide[pl.ds(0, 2 * n), :] = block.astype(f32)
        even = wide[pl.ds(0, n, stride=2), :].astype(bf16)
        odd = wide[pl.ds(1, n, stride=2), :].astype(bf16)
        return even, odd

    acc[...] = jnp.zeros_like(acc)

    def project(c, carry):
        cols = pl.ds(pl.multiple_of(c * CHUNK, CHUNK), CHUNK)
        rows = pl.ds(pl.multiple_of(c * 2 * CHUNK, 2 * CHUNK), 2 * CHUNK)
        pltpu.make_async_copy(prefix_hbm.at[:, cols], prefix_v.at[:, cols], load_sem.at[0, c]).wait()
        pltpu.make_async_copy(w_hbm.at[rows], w_v.at[rows], load_sem.at[1, c]).wait()
        wk, wv = halves(w_v[rows, :], CHUNK)
        acc[...] += dot(prefix_v[:, cols], jnp.concatenate([wk, wv], axis=1), ((1,), (0,)))
        return carry

    lax.fori_loop(0, AHEAD, project, 0)
    pl.semaphore_wait(barrier, 16)
    w_copies = []
    for by in (2, 1, 3):
        to = t_at(by)
        start = (to * 2 + core) * 2 * COLS + quarter * (COLS // 2)
        cp = pltpu.make_async_remote_copy(
            src_ref=w_hbm.at[pl.ds(pl.multiple_of(start, COLS // 2), COLS // 2)],
            dst_ref=wbuf.at[by - 1, quarter],
            send_sem=w_send.at[by - 1],
            recv_sem=w_recv.at[by - 1],
            device_id={"dp": d, "tensor": to},
            device_id_type=MESH,
        )
        cp.start()
        w_copies.append(cp)

    lax.fori_loop(AHEAD, CHUNKS, project, 0)
    near[REACH] = acc[...].astype(bf16)

    kv_copies = []
    for n, o in enumerate(OFFSETS):
        cp = pltpu.make_async_remote_copy(
            src_ref=near.at[REACH],
            dst_ref=near.at[REACH - o],
            send_sem=kv_send.at[n],
            recv_sem=kv_recv.at[n],
            device_id={"dp": dp_at(o), "tensor": t},
            device_id_type=MESH,
        )
        cp.start()
        kv_copies.append(cp)

    def pass_on(by, way):
        half = COLS // 4
        rows = (pl.ds(0, 2 * half), pl.ds(0, 2 * half), pl.ds(0, half), pl.ds(half, half))[way]
        return pltpu.make_async_remote_copy(
            src_ref=wbuf.at[by, quarter, rows],
            dst_ref=wbuf.at[by, quarter, rows],
            send_sem=pass_send.at[by, way],
            recv_sem=pass_recv.at[by, way],
            device_id={"dp": beside[way], "tensor": t},
            device_id_type=MESH,
        )

    first_own = bp_ref[0] == d
    own_slot = jnp.where(first_own, 0, 1)
    other_slot = 1 - own_slot
    other_index = lax.rem(jnp.where(first_own, bp_ref[1], bp_ref[0]) - d + REACH + dp_count, dp_count)

    for cp in loads:
        cp.wait()

    def take_answers(role, slot):
        keys, values = halves(kv_v[slot], ANS)
        kfull[role, pl.ds(PFX, ANS), :] = keys
        vt[role, :, pl.ds(PFX, ANS)] = values.T

    def take_prefix(role, block):
        kfull[role, pl.ds(0, PFX), :] = block[:, :HD]
        vpre[role] = block[:, HD:]
        vt[role, :, pl.ds(0, PFX)] = block[:, HD:].T

    take_answers(0, own_slot)
    take_answers(1, other_slot)
    take_prefix(0, near[REACH])
    kg[...] = jnp.zeros_like(kg)

    def attend(n, carry):
        @pl.when(n == FIRST)
        def _():
            for cp in kv_copies:
                cp.wait()
            take_prefix(1, near[jnp.minimum(other_index, WINDOW - 1)])

        @pl.when(n == PASS_AT)
        def _():
            for cp in w_copies:
                cp.wait()
            for by in range(3):
                for way in range(4):
                    pass_on(by, way).start()

        is_other = (n >= FIRST) & (n < FIRST + TURNS)
        role = jnp.where(is_other, 1, 0)
        turn = jnp.where(n < FIRST, n, jnp.where(is_other, n - FIRST, n - TURNS))
        slot = jnp.where(is_other, other_slot, own_slot)
        causal = lax.broadcasted_iota(jnp.int32, (HD, HD), 0) <= lax.broadcasted_iota(jnp.int32, (HD, HD), 1)

        def place_of(b):
            lanes = pl.ds(pl.multiple_of((turn * AT_ONCE + b // 2) * HD, HD), HD)
            return pl.ds((b % 2) * ROWS, ROWS), lanes, PFX + (b % 2 + 1) * ROWS

        def scores(b):
            rows, lanes, end = place_of(b)
            return dot(kfull[role, pl.ds(0, end), :], q_v[slot, rows, lanes], ((1,), (1,)))

        def softmax(s):
            fulls, halfs = [], []
            for part in range(ROWS // HD):
                end = s.shape[0] - ROWS + (part + 1) * HD
                own = s[:end, part * HD : (part + 1) * HD]
                tail = jnp.where(causal, own[end - HD :], -jnp.inf)
                own = jnp.concatenate([own[: end - HD], tail], axis=0)
                top = jnp.max(own, axis=0, keepdims=True)
                e = jnp.exp2((own - top) * (SCALING * LOG2E))
                full = e * (1.0 / jnp.sum(e, axis=0, keepdims=True))
                fulls.append(full[:PFX])
                half = full.astype(bf16)
                if end < s.shape[0]:
                    half = jnp.concatenate([half, jnp.zeros((s.shape[0] - end, HD), bf16)], axis=0)
                halfs.append(half)
            return jnp.concatenate(fulls, axis=1), jnp.concatenate(halfs, axis=1)

        def rest(b, full, half):
            rows, lanes, end = place_of(b)
            q, do = q_v[slot, rows, lanes], do_v[slot, rows, lanes]
            ctx = dot(vt[role, :, pl.ds(0, end)], half, ((1,), (0,)))
            res[role, rows, lanes] = ctx.astype(bf16).T
            grad = dot(vpre[role], do, ((1,), (1,)))
            delta = jnp.sum(do.T.astype(f32) * ctx, axis=0, keepdims=True)
            sg = (full * (grad - delta)).astype(bf16)
            kg[role, 0] += dot(sg, q, ((1,), (0,)))
            kg[role, 1] += dot(half[:PFX], do, ((1,), (0,)))

        count = 2 * AT_ONCE
        waiting = scores(0)
        done = None
        for b in range(count):
            now = waiting
            if b + 1 < count:
                waiting = scores(b + 1)
            probs = softmax(now)
            if done is not None:
                rest(b - 1, *done)
            done = probs
        rest(count - 1, *done)

        @pl.when(n == FIRST + TURNS - 1)
        def _():
            key_grad = (kg[1, 0] * SCALING).astype(bf16)
            value_grad = kg[1, 1].astype(bf16)
            zero = jnp.zeros((PFX, HD), bf16)
            for m, o in enumerate(OFFSETS):
                keep = other_index == o + REACH
                gsend[m, :, pl.ds(0, HD)] = lax.select(keep, key_grad, zero)
                gsend[m, :, pl.ds(HD, HD)] = lax.select(keep, value_grad, zero)
                grad_copy(m, o).start()

        return carry

    def grad_copy(m, o):
        return pltpu.make_async_remote_copy(
            src_ref=gsend.at[m],
            dst_ref=grecv.at[m],
            send_sem=gr_send.at[m],
            recv_sem=gr_recv.at[m],
            device_id={"dp": dp_at(o), "tensor": t},
            device_id_type=MESH,
        )

    lax.fori_loop(0, 2 * TURNS, attend, 0)

    def widen(by, b, block, part=None):
        n = CHUNK if part is None else CHUNK // 2
        wk, wv = halves(block, n)
        rows = pl.ds(b * CHUNK + (part or 0) * n, n)
        wfull[rows, pl.ds(by * 2 * HD, HD)] = wk
        wfull[rows, pl.ds(by * 2 * HD + HD, HD)] = wv

    for b in range(COLS // CHUNK):
        start = pl.multiple_of(unit * 2 * COLS + b * 2 * CHUNK, 2 * CHUNK)
        widen(0, b, w_v[pl.ds(start, 2 * CHUNK), :])
    local = (other_index == REACH).astype(f32)
    key_sum = (kg[0, 0] + kg[1, 0] * local) * SCALING
    value_sum = kg[0, 1] + kg[1, 1] * local
    for m, o in enumerate(OFFSETS):
        grad_copy(m, o).wait()
        key_sum = key_sum + grecv[m, :, pl.ds(0, HD)].astype(f32)
        value_sum = value_sum + grecv[m, :, pl.ds(HD, HD)].astype(f32)
    gbuf[0, 0, :, pl.ds(0, HD)] = key_sum.astype(bf16)
    gbuf[0, 0, :, pl.ds(HD, HD)] = value_sum.astype(bf16)

    def gather(cross, by):
        n = cross * 4 + by
        here_at = (t_count - by) % t_count
        return pltpu.make_async_remote_copy(
            src_ref=gbuf.at[0, by] if cross else gbuf.at[0, 0],
            dst_ref=gbuf.at[1, by] if cross else gbuf.at[0, here_at],
            send_sem=gt_send.at[n],
            recv_sem=gt_recv.at[n],
            device_id={"dp": sib, "tensor": t} if cross else {"dp": d, "tensor": t_at(by)},
            device_id_type=MESH,
        )

    for by in (2, 1, 3):
        gather(0, by).start()
    gather(1, 0).start()
    for by in (1, 3, 2):
        gather(0, (t_count - by) % t_count).wait_recv()
        gather(1, by).start()
    for by in range(3):
        for way in range(4):
            pass_on(by, way).wait()
    for by in (1, 2, 3):
        for b in range(COLS // CHUNK):
            for part in range(2):
                widen(by, b, wbuf[3 - by, 2 * b + part], part)
    for by in (1, 2, 3):
        gather(0, by).wait_send()
    for by in range(4):
        gather(1, by).wait()

    lhs = jnp.concatenate(
        [jnp.concatenate([gbuf[c, by] for by in range(4)], axis=1) for c in range(2)], axis=0
    )
    otile[...] = dot(lhs, wfull[...], ((1,), (1,))).astype(bf16).reshape(2, PFX, COLS)

    here = pl.ds(pl.multiple_of(unit * COLS, COLS), COLS)
    share = PFX // 4
    outs = []
    for n, (cross, by) in enumerate(((1, 2), (0, 2), (1, 1), (0, 1), (1, 3), (0, 3), (1, 0))):
        to = t_at(by)
        cp = pltpu.make_async_remote_copy(
            src_ref=otile.at[cross, pl.ds(pl.multiple_of(to * share, share), share)],
            dst_ref=pg.at[:, here],
            send_sem=pg_send.at[n],
            recv_sem=pg_recv.at[n],
            device_id={"dp": sib if cross else d, "tensor": to},
            device_id_type=MESH,
        )
        cp.start()
        outs.append(cp)
    pg[:, here] = otile[0, pl.ds(pl.multiple_of(t * share, share), share), :]
    for cp in outs:
        cp.wait()


def put_out(bp_ref, res, pg, attn_hbm, pg_hbm, sem):
    own_slot = jnp.where(bp_ref[0] == lax.axis_index("dp"), 0, 1)
    copies = [
        pltpu.make_async_copy(res.at[0], attn_hbm.at[own_slot], sem.at[0]),
        pltpu.make_async_copy(res.at[1], attn_hbm.at[1 - own_slot], sem.at[1]),
        pltpu.make_async_copy(pg, pg_hbm, sem.at[2]),
    ]
    for cp in copies:
        cp.start()
    for cp in copies:
        cp.wait()


def shards(prefix, kv_weight, ans_query, ans_kv, d_out, branch_prompt):
    t_count, dp_count = lax.axis_size("tensor"), lax.axis_size("dp")
    hbm = pl.BlockSpec(memory_space=pltpu.HBM)
    whole = pl.BlockSpec(memory_space=pltpu.VMEM)
    dma = pltpu.SemaphoreType.DMA
    vmem = pltpu.VMEM
    attn, pg = pl.pallas_call(
        functools.partial(kernel, dp_count, t_count),
        out_shape=(
            pltpu.VMEM((2, ANS, HEADS * HD), bf16),
            pltpu.VMEM((PFX // 4, D), bf16),
        ),
        in_specs=[pl.BlockSpec(memory_space=pltpu.SMEM)] + [hbm] * 5,
        out_specs=(whole, whole),
        scratch_shapes=[
            vmem((PFX, D), bf16),
            vmem((2 * D, HD), bf16),
            vmem((2, ANS, HEADS * HD), bf16),
            vmem((2, ANS, HEADS * HD), bf16),
            vmem((2, 2 * ANS, HD), bf16),
            vmem((2 * CHUNK, HD), f32),
            vmem((PFX, 2 * HD), f32),
            vmem((WINDOW, PFX, 2 * HD), bf16),
            vmem((2, PFX + ANS, HD), bf16),
            vmem((2, HD, PFX + ANS), bf16),
            vmem((2, PFX, HD), bf16),
            vmem((2, 2, PFX, HD), f32),
            vmem((2 * REACH, PFX, 2 * HD), bf16),
            vmem((2 * REACH, PFX, 2 * HD), bf16),
            vmem((2, 4, PFX, 2 * HD), bf16),
            vmem((3, 4, COLS // 2, HD), bf16),
            vmem((COLS, 4 * 2 * HD), bf16),
            vmem((2, PFX, COLS), bf16),
            dma((2, CHUNKS)),
            dma((3,)),
            dma((6,)),
            dma((6,)),
            dma((3,)),
            dma((3,)),
            dma((3, 4)),
            dma((3, 4)),
            dma((6,)),
            dma((6,)),
            dma((8,)),
            dma((8,)),
            dma((7,)),
            dma((7,)),
        ],
        compiler_params=pltpu.CompilerParams(
            collective_id=0, has_side_effects=True, vmem_limit_bytes=58 * 1024 * 1024
        ),
        name="prefix_step",
    )(
        branch_prompt,
        prefix.reshape(PFX, D),
        kv_weight.reshape(2 * D, HD),
        ans_query.reshape(2, ANS, HEADS * HD),
        ans_kv.reshape(2, 2 * ANS, HD),
        d_out.reshape(2, ANS, HEADS * HD),
    )
    attn, pg = pl.pallas_call(
        put_out,
        out_shape=(
            jax.ShapeDtypeStruct((2, ANS, HEADS * HD), bf16),
            jax.ShapeDtypeStruct((PFX // 4, D), bf16),
        ),
        in_specs=[pl.BlockSpec(memory_space=pltpu.SMEM), whole, whole],
        out_specs=(hbm, hbm),
        scratch_shapes=[dma((3,))],
        name="put_out",
    )(branch_prompt, pltpu.with_memory_space_constraint(attn, pltpu.VMEM), pltpu.with_memory_space_constraint(pg, pltpu.VMEM))
    return attn.reshape(2 * ANS, HEADS * HD), pg.reshape(1, PFX // 4, D)


def solution(mesh):
    return jax.shard_map(
        shards,
        mesh=mesh,
        in_specs=(
            P("dp", None, None),
            P(None, None, "tensor"),
            P("dp", "tensor"),
            P("dp", None, "tensor"),
            P("dp", "tensor"),
            P("dp"),
        ),
        out_specs=(P("dp", "tensor"), P("dp", "tensor", None)),
        check_vma=False,
    )
```

```python
import functools
import math

import jax
import jax.numpy as jnp
from jax import lax
from jax.experimental import pallas as pl
from jax.experimental.pallas import tpu as pltpu
from jax.sharding import PartitionSpec as P

MESH = pl.DeviceIdType.MESH
HD = 128
PFX = 128
ANS = 512
HEADS = 8
D = 8192
REACH = 3
WINDOW = 2 * REACH + 1
CHUNK = 512
CHUNKS = D // CHUNK
COLS = 1024
ROWS = 256
AT_ONCE = 4
TURNS = 2
FIRST = 2
PASS_AT = 2
AHEAD = 4
LOAD_AT = 9
PIECES = 2
X = 4
SCALING = HD ** (-0.5)
LOG2E = math.log2(math.e)
OFFSETS = [o for o in (3, -3, 2, -2, 1, -1)]
f32, bf16 = jnp.float32, jnp.bfloat16


def dot(a, b, dims):
    return lax.dot_general(a, b, (dims, ((), ())), preferred_element_type=f32)


def kernel(
    dp_count,
    t_count,
    bp_ref,
    prefix_hbm,
    w_hbm,
    q_hbm,
    kv_hbm,
    do_hbm,
    res,
    pg,
    prefix_v,
    w_v,
    q_v,
    do_v,
    kv_v,
    wide,
    acc,
    near,
    kfull,
    vt,
    vpre,
    kg,
    gsend,
    grecv,
    gbuf,
    wbuf,
    wfull,
    otile,
    load_sem,
    in_sem,
    kv_send,
    kv_recv,
    w_send,
    w_recv,
    pass_send,
    pass_recv,
    gr_send,
    gr_recv,
    gt_send,
    gt_recv,
    pg_send,
    pg_recv,
):
    d = lax.axis_index("dp")
    t = lax.axis_index("tensor")
    core = lax.rem(d, 2)
    sib = d + 1 - 2 * core
    unit = t * 2 + core

    def dp_at(by):
        return lax.rem(d + by + dp_count, dp_count)

    def t_at(by):
        return lax.rem(t + by, t_count)

    loads = []
    for c in range(CHUNKS):
        cols = pl.ds(c * CHUNK, CHUNK)
        rows = pl.ds(c * 2 * CHUNK, 2 * CHUNK)
        pltpu.make_async_copy(prefix_hbm.at[:, cols], prefix_v.at[:, cols], load_sem.at[0, c]).start()
        pltpu.make_async_copy(w_hbm.at[rows], w_v.at[rows], load_sem.at[1, c]).start()
    for n, (src, dst) in enumerate(((kv_hbm, kv_v), (q_hbm, q_v), (do_hbm, do_v))):
        loads.append(pltpu.make_async_copy(src, dst, in_sem.at[n]))

    chip = d // 2
    x, z = lax.rem(chip, X), chip // X
    quarter = lax.rem(z + 2 * x, 4)
    x_next = (z * X + lax.rem(x + 1, X)) * 2 + core
    x_last = (z * X + lax.rem(x + X - 1, X)) * 2 + core
    beside = (dp_at(2 * X), dp_at(-2 * X), x_next, x_last)

    barrier = pltpu.get_barrier_semaphore()
    for o in OFFSETS:
        pl.semaphore_signal(barrier, inc=1, device_id={"dp": dp_at(o), "tensor": t}, device_id_type=MESH)
    for by in range(1, 4):
        pl.semaphore_signal(barrier, inc=1, device_id={"dp": d, "tensor": t_at(by)}, device_id_type=MESH)
        pl.semaphore_signal(barrier, inc=1, device_id={"dp": sib, "tensor": t_at(by)}, device_id_type=MESH)
    for to in beside:
        pl.semaphore_signal(barrier, inc=1, device_id={"dp": to, "tensor": t}, device_id_type=MESH)
    def halves(block, n):
        wide[pl.ds(0, 2 * n), :] = block.astype(f32)
        even = wide[pl.ds(0, n, stride=2), :].astype(bf16)
        odd = wide[pl.ds(1, n, stride=2), :].astype(bf16)
        return even, odd

    acc[...] = jnp.zeros_like(acc)

    def project(c, carry):
        cols = pl.ds(pl.multiple_of(c * CHUNK, CHUNK), CHUNK)
        rows = pl.ds(pl.multiple_of(c * 2 * CHUNK, 2 * CHUNK), 2 * CHUNK)
        pltpu.make_async_copy(prefix_hbm.at[:, cols], prefix_v.at[:, cols], load_sem.at[0, c]).wait()
        pltpu.make_async_copy(w_hbm.at[rows], w_v.at[rows], load_sem.at[1, c]).wait()
        wk, wv = halves(w_v[rows, :], CHUNK)
        acc[...] += dot(prefix_v[:, cols], jnp.concatenate([wk, wv], axis=1), ((1,), (0,)))
        return carry

    lax.fori_loop(0, AHEAD, project, 0)
    pl.semaphore_wait(barrier, 16)
    w_copies = []
    for by in (2, 1, 3):
        to = t_at(by)
        start = (to * 2 + core) * 2 * COLS + quarter * (COLS // 2)
        cp = pltpu.make_async_remote_copy(
            src_ref=w_hbm.at[pl.ds(pl.multiple_of(start, COLS // 2), COLS // 2)],
            dst_ref=wbuf.at[by - 1, quarter],
            send_sem=w_send.at[by - 1],
            recv_sem=w_recv.at[by - 1],
            device_id={"dp": d, "tensor": to},
            device_id_type=MESH,
        )
        cp.start()
        w_copies.append(cp)

    lax.fori_loop(AHEAD, LOAD_AT, project, 0)
    for cp in loads:
        cp.start()
    lax.fori_loop(LOAD_AT, CHUNKS, project, 0)
    near[REACH] = acc[...].astype(bf16)

    kv_copies = []
    for n, o in enumerate(OFFSETS):
        cp = pltpu.make_async_remote_copy(
            src_ref=near.at[REACH],
            dst_ref=near.at[REACH - o],
            send_sem=kv_send.at[n],
            recv_sem=kv_recv.at[n],
            device_id={"dp": dp_at(o), "tensor": t},
            device_id_type=MESH,
        )
        cp.start()
        kv_copies.append(cp)

    def pass_on(by, way):
        half = COLS // 4
        rows = (pl.ds(0, 2 * half), pl.ds(0, 2 * half), pl.ds(0, half), pl.ds(half, half))[way]
        return pltpu.make_async_remote_copy(
            src_ref=wbuf.at[by, quarter, rows],
            dst_ref=wbuf.at[by, quarter, rows],
            send_sem=pass_send.at[by, way],
            recv_sem=pass_recv.at[by, way],
            device_id={"dp": beside[way], "tensor": t},
            device_id_type=MESH,
        )

    first_own = bp_ref[0] == d
    own_slot = jnp.where(first_own, 0, 1)
    other_slot = 1 - own_slot
    other_index = lax.rem(jnp.where(first_own, bp_ref[1], bp_ref[0]) - d + REACH + dp_count, dp_count)

    for cp in loads:
        cp.wait()

    def take_answers(role, slot):
        keys, values = halves(kv_v[slot], ANS)
        kfull[role, pl.ds(PFX, ANS), :] = keys
        vt[role, :, pl.ds(PFX, ANS)] = values.T

    def take_prefix(role, block):
        kfull[role, pl.ds(0, PFX), :] = block[:, :HD]
        vpre[role] = block[:, HD:]
        vt[role, :, pl.ds(0, PFX)] = block[:, HD:].T

    take_answers(0, own_slot)
    take_answers(1, other_slot)
    take_prefix(0, near[REACH])
    kg[...] = jnp.zeros_like(kg)

    def attend(n, carry):
        @pl.when(n == FIRST)
        def _():
            for cp in kv_copies:
                cp.wait()
            take_prefix(1, near[jnp.minimum(other_index, WINDOW - 1)])

        @pl.when(n == PASS_AT - 1)
        def _():
            for cp in w_copies[1:]:
                cp.wait()
            for by in (0, 2):
                for way in range(4):
                    pass_on(by, way).start()

        @pl.when(n == PASS_AT + 1)
        def _():
            w_copies[0].wait()
            for way in range(4):
                pass_on(1, way).start()

        is_other = (n >= FIRST) & (n < FIRST + TURNS)
        role = jnp.where(is_other, 1, 0)
        turn = jnp.where(n < FIRST, n, jnp.where(is_other, n - FIRST, n - TURNS))
        slot = jnp.where(is_other, other_slot, own_slot)
        causal = lax.broadcasted_iota(jnp.int32, (HD, HD), 0) <= lax.broadcasted_iota(jnp.int32, (HD, HD), 1)

        def place_of(b):
            lanes = pl.ds(pl.multiple_of((turn * AT_ONCE + b // 2) * HD, HD), HD)
            return pl.ds((b % 2) * ROWS, ROWS), lanes, PFX + (b % 2 + 1) * ROWS

        def scores(b):
            rows, lanes, end = place_of(b)
            return dot(kfull[role, pl.ds(0, end), :], q_v[slot, rows, lanes], ((1,), (1,)))

        def softmax(s):
            fulls, halfs = [], []
            for part in range(ROWS // HD):
                end = s.shape[0] - ROWS + (part + 1) * HD
                own = s[:end, part * HD : (part + 1) * HD]
                tail = jnp.where(causal, own[end - HD :], -jnp.inf)
                own = jnp.concatenate([own[: end - HD], tail], axis=0)
                top = jnp.max(own, axis=0, keepdims=True)
                e = jnp.exp2((own - top) * (SCALING * LOG2E))
                full = e * (1.0 / jnp.sum(e, axis=0, keepdims=True))
                fulls.append(full[:PFX])
                half = full.astype(bf16)
                if end < s.shape[0]:
                    half = jnp.concatenate([half, jnp.zeros((s.shape[0] - end, HD), bf16)], axis=0)
                halfs.append(half)
            return jnp.concatenate(fulls, axis=1), jnp.concatenate(halfs, axis=1)

        def rest(b, full, half):
            rows, lanes, end = place_of(b)
            q, do = q_v[slot, rows, lanes], do_v[slot, rows, lanes]
            ctx = dot(vt[role, :, pl.ds(0, end)], half, ((1,), (0,)))
            res[role, rows, lanes] = ctx.astype(bf16).T
            grad = dot(vpre[role], do, ((1,), (1,)))
            delta = jnp.sum(do.T.astype(f32) * ctx, axis=0, keepdims=True)
            sg = (full * (grad - delta)).astype(bf16)
            kg[role, 0] += dot(sg, q, ((1,), (0,)))
            kg[role, 1] += dot(half[:PFX], do, ((1,), (0,)))

        count = 2 * AT_ONCE
        waiting = scores(0)
        done = None
        for b in range(count):
            now = waiting
            if b + 1 < count:
                waiting = scores(b + 1)
            probs = softmax(now)
            if done is not None:
                rest(b - 1, *done)
            done = probs
        rest(count - 1, *done)

        @pl.when(n == FIRST + TURNS - 1)
        def _():
            key_grad = (kg[1, 0] * SCALING).astype(bf16)
            value_grad = kg[1, 1].astype(bf16)
            zero = jnp.zeros((PFX, HD), bf16)
            for m, o in enumerate(OFFSETS):
                keep = other_index == o + REACH
                gsend[m, :, pl.ds(0, HD)] = lax.select(keep, key_grad, zero)
                gsend[m, :, pl.ds(HD, HD)] = lax.select(keep, value_grad, zero)
                grad_copy(m, o).start()

        return carry

    def grad_copy(m, o):
        return pltpu.make_async_remote_copy(
            src_ref=gsend.at[m],
            dst_ref=grecv.at[m],
            send_sem=gr_send.at[m],
            recv_sem=gr_recv.at[m],
            device_id={"dp": dp_at(o), "tensor": t},
            device_id_type=MESH,
        )

    lax.fori_loop(0, 2 * TURNS, attend, 0)

    def widen(by, b, block, part=None):
        n = CHUNK if part is None else CHUNK // 2
        wk, wv = halves(block, n)
        rows = pl.ds(b * CHUNK + (part or 0) * n, n)
        wfull[rows, pl.ds(by * 2 * HD, HD)] = wk
        wfull[rows, pl.ds(by * 2 * HD + HD, HD)] = wv

    for b in range(COLS // CHUNK):
        start = pl.multiple_of(unit * 2 * COLS + b * 2 * CHUNK, 2 * CHUNK)
        widen(0, b, w_v[pl.ds(start, 2 * CHUNK), :])
    local = (other_index == REACH).astype(f32)
    key_sum = (kg[0, 0] + kg[1, 0] * local) * SCALING
    value_sum = kg[0, 1] + kg[1, 1] * local
    for m, o in enumerate(OFFSETS):
        grad_copy(m, o).wait()
        key_sum = key_sum + grecv[m, :, pl.ds(0, HD)].astype(f32)
        value_sum = value_sum + grecv[m, :, pl.ds(HD, HD)].astype(f32)
    gbuf[0, 0, :, pl.ds(0, HD)] = key_sum.astype(bf16)
    gbuf[0, 0, :, pl.ds(HD, HD)] = value_sum.astype(bf16)

    def gather(cross, by):
        n = cross * 4 + by
        here_at = (t_count - by) % t_count
        return pltpu.make_async_remote_copy(
            src_ref=gbuf.at[0, by] if cross else gbuf.at[0, 0],
            dst_ref=gbuf.at[1, by] if cross else gbuf.at[0, here_at],
            send_sem=gt_send.at[n],
            recv_sem=gt_recv.at[n],
            device_id={"dp": sib, "tensor": t} if cross else {"dp": d, "tensor": t_at(by)},
            device_id_type=MESH,
        )

    for by in (2, 1, 3):
        gather(0, by).start()
    gather(1, 0).start()
    for by in (1, 3, 2):
        gather(0, (t_count - by) % t_count).wait_recv()
        gather(1, by).start()
    for by in range(3):
        for way in range(4):
            pass_on(by, way).wait()
    for by in (1, 2, 3):
        for b in range(COLS // CHUNK):
            for part in range(2):
                widen(by, b, wbuf[3 - by, 2 * b + part], part)
    for by in (1, 2, 3):
        gather(0, by).wait_send()
    for by in range(4):
        gather(1, by).wait()

    lhs = jnp.concatenate(
        [jnp.concatenate([gbuf[c, by] for by in range(4)], axis=1) for c in range(2)], axis=0
    )
    share = PFX // 4
    mine = pl.ds(pl.multiple_of(t * share, share), share)
    outs = []
    for piece in range(PIECES):
        width = COLS // PIECES
        part = pl.ds(piece * width, width)
        here = pl.ds(pl.multiple_of(unit * COLS + piece * width, width), width)
        rows = dot(lhs, wfull[part, :], ((1,), (1,))).astype(bf16)
        otile[:, :, part] = rows.reshape(2, PFX, width)
        for n, (cross, by) in enumerate(((1, 2), (0, 2), (1, 1), (0, 1), (1, 3), (0, 3), (1, 0))):
            to = t_at(by)
            cp = pltpu.make_async_remote_copy(
                src_ref=otile.at[cross, pl.ds(pl.multiple_of(to * share, share), share), part],
                dst_ref=pg.at[:, here],
                send_sem=pg_send.at[piece, n],
                recv_sem=pg_recv.at[piece, n],
                device_id={"dp": sib if cross else d, "tensor": to},
                device_id_type=MESH,
            )
            cp.start()
            outs.append(cp)
        pg[:, here] = otile[0, mine, part]
    for cp in outs:
        cp.wait()


def put_out(bp_ref, res, pg, attn_hbm, pg_hbm, sem):
    own_slot = jnp.where(bp_ref[0] == lax.axis_index("dp"), 0, 1)
    copies = [
        pltpu.make_async_copy(res.at[0], attn_hbm.at[own_slot], sem.at[0]),
        pltpu.make_async_copy(res.at[1], attn_hbm.at[1 - own_slot], sem.at[1]),
        pltpu.make_async_copy(pg, pg_hbm, sem.at[2]),
    ]
    for cp in copies:
        cp.start()
    for cp in copies:
        cp.wait()


def shards(prefix, kv_weight, ans_query, ans_kv, d_out, branch_prompt):
    t_count, dp_count = lax.axis_size("tensor"), lax.axis_size("dp")
    hbm = pl.BlockSpec(memory_space=pltpu.HBM)
    whole = pl.BlockSpec(memory_space=pltpu.VMEM)
    dma = pltpu.SemaphoreType.DMA
    vmem = pltpu.VMEM
    attn, pg = pl.pallas_call(
        functools.partial(kernel, dp_count, t_count),
        out_shape=(
            pltpu.VMEM((2, ANS, HEADS * HD), bf16),
            pltpu.VMEM((PFX // 4, D), bf16),
        ),
        in_specs=[pl.BlockSpec(memory_space=pltpu.SMEM)] + [hbm] * 5,
        out_specs=(whole, whole),
        scratch_shapes=[
            vmem((PFX, D), bf16),
            vmem((2 * D, HD), bf16),
            vmem((2, ANS, HEADS * HD), bf16),
            vmem((2, ANS, HEADS * HD), bf16),
            vmem((2, 2 * ANS, HD), bf16),
            vmem((2 * CHUNK, HD), f32),
            vmem((PFX, 2 * HD), f32),
            vmem((WINDOW, PFX, 2 * HD), bf16),
            vmem((2, PFX + ANS, HD), bf16),
            vmem((2, HD, PFX + ANS), bf16),
            vmem((2, PFX, HD), bf16),
            vmem((2, 2, PFX, HD), f32),
            vmem((2 * REACH, PFX, 2 * HD), bf16),
            vmem((2 * REACH, PFX, 2 * HD), bf16),
            vmem((2, 4, PFX, 2 * HD), bf16),
            vmem((3, 4, COLS // 2, HD), bf16),
            vmem((COLS, 4 * 2 * HD), bf16),
            vmem((2, PFX, COLS), bf16),
            dma((2, CHUNKS)),
            dma((3,)),
            dma((6,)),
            dma((6,)),
            dma((3,)),
            dma((3,)),
            dma((3, 4)),
            dma((3, 4)),
            dma((6,)),
            dma((6,)),
            dma((8,)),
            dma((8,)),
            dma((PIECES, 7)),
            dma((PIECES, 7)),
        ],
        compiler_params=pltpu.CompilerParams(
            collective_id=0, has_side_effects=True, vmem_limit_bytes=58 * 1024 * 1024
        ),
        name="prefix_step",
    )(
        branch_prompt,
        prefix.reshape(PFX, D),
        kv_weight.reshape(2 * D, HD),
        ans_query.reshape(2, ANS, HEADS * HD),
        ans_kv.reshape(2, 2 * ANS, HD),
        d_out.reshape(2, ANS, HEADS * HD),
    )
    attn, pg = pl.pallas_call(
        put_out,
        out_shape=(
            jax.ShapeDtypeStruct((2, ANS, HEADS * HD), bf16),
            jax.ShapeDtypeStruct((PFX // 4, D), bf16),
        ),
        in_specs=[pl.BlockSpec(memory_space=pltpu.SMEM), whole, whole],
        out_specs=(hbm, hbm),
        scratch_shapes=[dma((3,))],
        name="put_out",
    )(branch_prompt, pltpu.with_memory_space_constraint(attn, pltpu.VMEM), pltpu.with_memory_space_constraint(pg, pltpu.VMEM))
    return attn.reshape(2 * ANS, HEADS * HD), pg.reshape(1, PFX // 4, D)


def solution(mesh):
    return jax.shard_map(
        shards,
        mesh=mesh,
        in_specs=(
            P("dp", None, None),
            P(None, None, "tensor"),
            P("dp", "tensor"),
            P("dp", None, "tensor"),
            P("dp", "tensor"),
            P("dp"),
        ),
        out_specs=(P("dp", "tensor"), P("dp", "tensor", None)),
        check_vma=False,
    )
```
